32 devices in a mesh: dp: 4 (over y, x), tensor: 8 (over z, core).
Axes of the slice: x: 2, y: 2, z: 4, core: 2. Of those that a mesh axis runs over, the one named last changes fastest.
Arguments:
- queries: bfloat16 [1536, 8192], P('dp', 'tensor'), may hold values from -180 to 180
- keys: bfloat16 [1536, 1024], P('dp'), may hold values from -4.5 to 4.5
- values: bfloat16 [1536, 1024], P('dp'), may hold values from -6 to 6
- grad_out: bfloat16 [1536, 8192], P('dp', 'tensor'), may hold values from -3 to 3
- weight: float32 [8192, 8192], P('dp', 'tensor'), as said below
- first_code: bfloat16 [8192, 8192], P('dp', 'tensor'), may hold values from -1 to 1, as said below
- first_rows: float32 [8192], P('dp'), may hold values from 0.2 to 5
- first_cols: float32 [8192], P('tensor'), may hold values from 0.2 to 5
- second_code: bfloat16 [8192, 8192], P('dp', 'tensor'), may hold values from 0 to 1, as said below
- second_rows: float32 [8192], P('dp'), may hold values from 0.5 to 20
- second_cols: float32 [8192], P('tensor'), may hold values from 0.5 to 20
Outputs:
- grad_queries: bfloat16 [1536, 8192], P('dp', 'tensor')
- new_weight: float32 [8192, 8192], P('dp', 'tensor')
- next_first_code: bfloat16 [8192, 8192], P('dp', 'tensor')
- next_first_rows: float32 [8192], P('dp')
- next_first_cols: float32 [8192], P('tensor')
- next_second_code: bfloat16 [8192, 8192], P('dp', 'tensor')
- next_second_rows: float32 [8192], P('dp')
- next_second_cols: float32 [8192], P('tensor')
The draws below stay inside these ranges and needn't reach their ends.
Inputs may be any that keep to these rules, and one draw needn't show every extreme that they name: `weight`: rows 8192 onward are zero. `first_code`: rows 8192 onward are zero. `second_code`: rows 8192 onward are zero; all other entries are 0.05 or more.
All inputs are finite; a program needn't handle non-finite values.
Results may differ from the reference program's by a relative error of at most 0.023.
Values may be sent and summed in bfloat16 or wider, within the bound.
A program may use at most 128 MiB of HBM per device.

```python
import math
import jax
import jax.numpy as jnp
from jax import lax

D = 8192
H = 64
KVH = 8
HD = 128
SEQ = 384
TOK = 1536
CPAD = 8192


def paired_draw(key):
    count = TOK // SEQ
    queries = jnp.clip(jax.random.normal(jax.random.fold_in(key, 101), (count, SEQ, H * HD), jnp.float32), -4.5, 4.5)
    keys = jnp.clip(jax.random.normal(jax.random.fold_in(key, 102), (count, SEQ, KVH * HD), jnp.float32), -4.5, 4.5)
    return (queries.reshape(TOK, H * HD), keys.reshape(TOK, KVH * HD))


def draw_queries(key, part):
    return paired_draw(key)[0].astype(jnp.bfloat16)


def draw_keys(key, part):
    return paired_draw(key)[1].astype(jnp.bfloat16)


def real_rows():
    return jnp.arange(CPAD)[:, None] < D


def draw_weight(key, part):
    filled = jax.random.normal(key, (CPAD, H * HD), jnp.float32) * (H * HD) ** (-0.5)
    return jnp.where(real_rows(), filled, 0.0)


def draw_first_code(key, part):
    filled = jax.random.uniform(key, (CPAD, H * HD), jnp.float32, -1.0, 1.0)
    return jnp.where(real_rows(), filled, 0.0).astype(jnp.bfloat16)


def draw_second_code(key, part):
    filled = jax.random.uniform(key, (CPAD, H * HD), jnp.float32, 0.05, 1.0)
    return jnp.where(real_rows(), filled, 0.0).astype(jnp.bfloat16)


def levels(rng, dims, shards, smallest, largest):
    def one(position, parts):
        draws = jax.random.uniform(jax.random.fold_in(jax.random.fold_in(rng, 6), position), (parts,), jnp.float32, smallest / len(shards), largest / len(shards))
        return jnp.repeat(jnp.exp(draws), dims[position] // parts).reshape((-1,) + (1,) * (len(dims) - position - 1))

    loudness = one(*shards[0])
    for cut in shards[1:]:
        loudness = loudness * one(*cut)
    return loudness


def scatter_about(key, dims, spread, most, split=(), dtype=jnp.bfloat16):
    level = levels(key, dims, split, -0.22, 0.18) if split else 1.0
    array = jax.random.normal(key, dims, jnp.float32) * spread * level
    return jnp.minimum(jnp.maximum(array, -most), most).astype(dtype)


def setup_inputs(seed: int = 0) -> dict:
    streams_of = jax.random.split(jax.random.key(seed), 12)
    return {
        "queries": draw_queries(jax.random.fold_in(streams_of[11], 71), 0),
        "keys": draw_keys(jax.random.fold_in(streams_of[11], 71), 0),
        "values": scatter_about(streams_of[2], (TOK, KVH * HD), 1.0, 6.0, ((0, 4),)),
        "grad_out": scatter_about(streams_of[3], (TOK, D), 0.5, 3.0, ((0, 4), (1, 8))),
        "weight": draw_weight(jax.random.fold_in(streams_of[11], 71), 0),
        "first_code": draw_first_code(jax.random.fold_in(streams_of[11], 71), 0),
        "first_rows": jnp.clip(jnp.exp(math.log(5.0) - 3.218876 * jax.random.uniform(streams_of[6], (CPAD,), jnp.float32) ** levels(streams_of[6], (CPAD,), ((0, 4),), -0.2, 0.2)), 0.2, 5.0),
        "first_cols": jnp.clip(jnp.exp(math.log(5.0) - 3.218876 * jax.random.uniform(streams_of[7], (H * HD,), jnp.float32) ** levels(streams_of[7], (H * HD,), ((0, 8),), -0.2, 0.2)), 0.2, 5.0),
        "second_code": draw_second_code(jax.random.fold_in(streams_of[11], 71), 0),
        "second_rows": jnp.clip(jnp.exp(math.log(20.0) - 3.6888795 * jax.random.uniform(streams_of[9], (CPAD,), jnp.float32) ** levels(streams_of[9], (CPAD,), ((0, 4),), -0.2, 0.2)), 0.5, 20.0),
        "second_cols": jnp.clip(jnp.exp(math.log(20.0) - 3.6888795 * jax.random.uniform(streams_of[10], (H * HD,), jnp.float32) ** levels(streams_of[10], (H * HD,), ((0, 8),), -0.2, 0.2)), 0.5, 20.0),
    }


beta_first = 0.9
beta_second = 0.95
learning = 0.01
decay_rate = 0.1
adam_eps = 1e-08
code_eps = 1e-06
correct_first = 1.0 - 0.9 ** 10
correct_second = 1.0 - 0.95 ** 10

def reference(queries, keys, values, grad_out, weight, first_code, first_rows, first_cols, second_code, second_rows, second_cols):
    count = queries.shape[0] // SEQ
    group = H // KVH
    factor = HD ** (-0.5)
    weight_half = weight.astype(jnp.bfloat16)
    grad_att = jnp.dot(grad_out, weight_half[:D], preferred_element_type=jnp.float32)
    grad_half = grad_att.astype(jnp.bfloat16)
    future = jnp.arange(SEQ)[None, :] > jnp.arange(SEQ)[:, None]

    def per_sequence(inputs):
        query_block, key_block, value_block, grad_block = inputs
        query_heads = query_block.reshape(SEQ, H, HD).astype(jnp.float32)
        key_heads = jnp.repeat(key_block.reshape(SEQ, KVH, HD), group, axis=1).astype(jnp.float32)
        value_heads = jnp.repeat(value_block.reshape(SEQ, KVH, HD), group, axis=1).astype(jnp.float32)
        scores = jnp.einsum('qhd,khd->hqk', query_heads, key_heads) * factor
        scores = jnp.where(future[None], -1e+30, scores)
        highest = lax.optimization_barrier(jnp.max(scores, axis=-1, keepdims=True))
        exponent = jnp.exp(scores - highest)
        probabilities = exponent / lax.optimization_barrier(jnp.sum(exponent, axis=-1, keepdims=True))
        weights_half = probabilities.astype(jnp.bfloat16)
        attended = jnp.einsum('hqk,khd->qhd', weights_half.astype(jnp.float32), value_heads).astype(jnp.bfloat16)
        grad_heads = grad_block.reshape(SEQ, H, HD).astype(jnp.float32)
        grad_probs = jnp.einsum('qhd,khd->hqk', grad_heads, value_heads)
        row_dot = lax.optimization_barrier(jnp.sum(grad_heads * attended.astype(jnp.float32), axis=-1))
        grad_scores = (probabilities * (grad_probs - row_dot.T[:, :, None])).astype(jnp.bfloat16)
        grad_query = (jnp.einsum('hqk,khd->qhd', grad_scores.astype(jnp.float32), key_heads) * factor).astype(jnp.bfloat16)
        return (grad_query.reshape(SEQ, H * HD), attended.reshape(SEQ, H * HD))
    grad_queries, attended = lax.map(per_sequence, (queries.reshape(count, SEQ, H * HD), keys.reshape(count, SEQ, KVH * HD), values.reshape(count, SEQ, KVH * HD), grad_half.reshape(count, SEQ, H * HD)))

    def accumulate(total, inputs):
        grad_block, att_block = inputs
        term = jnp.dot(grad_block.T, att_block, preferred_element_type=jnp.float32)
        return (total + lax.optimization_barrier(term.astype(jnp.bfloat16)).astype(jnp.float32), 0)
    weight_grad, unused = lax.scan(accumulate, jnp.zeros((D, H * HD), jnp.float32), (grad_out.reshape(count, SEQ, D), attended))
    weight_grad = jnp.pad(weight_grad, ((0, CPAD - D), (0, 0)))
    first = first_code.astype(jnp.float32) * jnp.minimum(first_rows[:, None], first_cols[None, :])
    second = second_code.astype(jnp.float32) * jnp.minimum(second_rows[:, None], second_cols[None, :])
    first_new = beta_first * first + (1.0 - beta_first) * weight_grad
    second_new = beta_second * second + (1.0 - beta_second) * weight_grad * weight_grad
    step_size = first_new / correct_first / (jnp.sqrt(second_new / correct_second) + adam_eps)
    new_weight = weight - learning * (step_size + decay_rate * weight)
    first_abs = jnp.abs(first_new)
    second_abs = jnp.abs(second_new)
    next_first_rows = lax.optimization_barrier(jnp.max(first_abs, axis=1))
    next_first_cols = lax.optimization_barrier(jnp.max(first_abs, axis=0))
    next_second_rows = lax.optimization_barrier(jnp.max(second_abs, axis=1))
    next_second_cols = lax.optimization_barrier(jnp.max(second_abs, axis=0))
    next_first_code = (first_new / (jnp.minimum(next_first_rows[:, None], next_first_cols[None, :]) + code_eps)).astype(jnp.bfloat16)
    next_second_code = (second_new / (jnp.minimum(next_second_rows[:, None], next_second_cols[None, :]) + code_eps)).astype(jnp.bfloat16)
    return (grad_queries.reshape(count * SEQ, H * HD), new_weight, next_first_code, next_first_rows, next_first_cols, next_second_code, next_second_rows, next_second_cols)
```

```python
import functools

import jax
import jax.numpy as jnp
from jax import lax
from jax.experimental import pallas as pl
from jax.experimental.pallas import tpu as pltpu
from jax.sharding import PartitionSpec as P

H = 64
KVH = 8
HD = 128


beta_first = 0.9
beta_second = 0.95
learning = 0.01
decay_rate = 0.1
adam_eps = 1e-08
code_eps = 1e-06
correct_first = 1.0 - 0.9**10
correct_second = 1.0 - 0.95**10


def attend(queries, key_sel, value_sel, heads_dev):
    length = queries.shape[0]
    query_heads = queries.reshape(length, heads_dev, HD)
    scores = jnp.einsum(
        "qhd,kd->hqk", query_heads, key_sel, preferred_element_type=jnp.float32
    ) * HD ** (-0.5)
    future = lax.broadcasted_iota(jnp.int32, (length, length), 1) > lax.broadcasted_iota(
        jnp.int32, (length, length), 0
    )
    scores = jnp.where(future[None], -1e30, scores)
    highest = jnp.max(scores, axis=-1, keepdims=True)
    exponent = jnp.exp(scores - highest)
    probabilities = exponent / jnp.sum(exponent, axis=-1, keepdims=True)
    weights_half = probabilities.astype(jnp.bfloat16)
    attended = jnp.einsum(
        "hqk,kd->qhd", weights_half, value_sel, preferred_element_type=jnp.float32
    )
    return (probabilities, attended.astype(jnp.bfloat16).reshape(length, heads_dev * HD))


def attend_back(probabilities, attended, grad_half, key_sel, value_sel, heads_dev):
    length = grad_half.shape[0]
    grad_heads = grad_half.reshape(length, heads_dev, HD)
    grad_probs = jnp.einsum(
        "qhd,kd->hqk", grad_heads, value_sel, preferred_element_type=jnp.float32
    )
    row_dot = jnp.sum(
        grad_heads.astype(jnp.float32)
        * attended.reshape(length, heads_dev, HD).astype(jnp.float32),
        axis=-1,
    )
    grad_scores = (probabilities * (grad_probs - row_dot.T[:, :, None])).astype(jnp.bfloat16)
    grad_query = jnp.einsum(
        "hqk,kd->qhd", grad_scores, key_sel, preferred_element_type=jnp.float32
    ) * HD ** (-0.5)
    return grad_query.astype(jnp.bfloat16).reshape(length, heads_dev * HD)


CORES = 2


def maxima_kernel(nd, nt, r_ref, c_ref, ro_ref, co_ref, rbuf, cbuf, rs, rr, cs, cr):
    d = lax.axis_index("dp")
    t = lax.axis_index("tensor")
    barrier = pltpu.get_barrier_semaphore()
    for o in range(1, nt):
        pl.semaphore_signal(barrier, inc=1, device_id={"tensor": (t + o) % nt})
    for o in range(1, nd):
        pl.semaphore_signal(barrier, inc=1, device_id={"dp": (d + o) % nd})
    pl.semaphore_wait(barrier, nt + nd - 2)
    copies = [
        pltpu.make_async_remote_copy(
            r_ref, rbuf.at[o], rs.at[o], rr.at[o], device_id={"tensor": (t + o) % nt}
        )
        for o in range(1, nt)
    ] + [
        pltpu.make_async_remote_copy(
            c_ref, cbuf.at[o], cs.at[o], cr.at[o], device_id={"dp": (d + o) % nd}
        )
        for o in range(1, nd)
    ]
    for copy in copies:
        copy.start()
    for copy in copies:
        copy.wait()
    rows = r_ref[...]
    for o in range(1, nt):
        rows = jnp.maximum(rows, rbuf[o])
    ro_ref[...] = rows
    cols = c_ref[...]
    for o in range(1, nd):
        cols = jnp.maximum(cols, cbuf[o])
    co_ref[...] = cols


def maxima(rows, cols, nd, nt):
    dma = pltpu.SemaphoreType.DMA
    vmem = pl.BlockSpec(memory_space=pltpu.VMEM)
    return pl.pallas_call(
        functools.partial(maxima_kernel, nd, nt),
        out_shape=(
            jax.ShapeDtypeStruct(rows.shape, rows.dtype),
            jax.ShapeDtypeStruct(cols.shape, cols.dtype),
        ),
        in_specs=[vmem] * 2,
        out_specs=(vmem,) * 2,
        scratch_shapes=[
            pltpu.VMEM((nt,) + rows.shape, rows.dtype),
            pltpu.VMEM((nd,) + cols.shape, cols.dtype),
            dma((nt,)),
            dma((nt,)),
            dma((nd,)),
            dma((nd,)),
        ],
        compiler_params=pltpu.CompilerParams(collective_id=1, has_side_effects=True),
    )(rows, cols)


PARTS = 3
HALVES = 2


def halves(width):
    return [pl.ds(k * (width // HALVES), width // HALVES) for k in range(HALVES)]


def fused_kernel(
    nd, nz,
    q_ref, k_ref, v_ref, grad_ref, w_hbm, fc_hbm, sc_hbm, fr_ref, fcol_ref, sr_ref, scol_ref,
    gq_ref, fn_hbm, sn_hbm, rmax_ref, cmax_ref,
    zbuf, g, gt, a, wh, stage, partial, r1, r2, mid, prob, fcv, scv, rb1, rb2,
    rloc, cloc, cacc, rbuf, cbuf, kv_k, kv_v,
    up_send, down_send, z_recv, own_send, d_send, d_recv, p_send, p_recv,
    a_send, a_recv, f_send, s1_send, s1_recv, s2_send, s2_recv,
    w_sem, c_sem, o_sem, rs, rr, cs, cr,
):
    d = lax.axis_index("dp")
    t = lax.axis_index("tensor")
    z = t // CORES
    c = t % CORES
    partner = t + 1 - 2 * c
    xn = d + 1 - 2 * (d % 2)
    yn = (d + 2) % 4
    dg = 3 - d
    length, width = grad_ref.shape
    rows = length // PARTS
    heads = width // HD
    total = w_hbm.shape[0]
    nt = CORES * nz
    has_up = z < nz - 1
    has_down = z > 0
    tile = stage.shape[1]
    tiles = total // tile
    far = jnp.abs(z - d)
    alpha, beta = halves(width)
    chunks = range(PARTS)
    scale = HD ** (-0.5)

    fetch_w = [
        pltpu.make_async_copy(w_hbm.at[pl.ds(i * tile, tile)], stage.at[i % 2], w_sem.at[i % 2])
        for i in range(tiles)
    ]
    fetch_c = [
        pltpu.make_async_copy(fc_hbm, fcv, c_sem.at[0]),
        pltpu.make_async_copy(sc_hbm, scv, c_sem.at[1]),
    ]
    fetch_w[0].start()
    fetch_w[1].start()

    barrier = pltpu.get_barrier_semaphore()
    for o in range(1, nt):
        pl.semaphore_signal(barrier, inc=1, device_id={"tensor": (t + o) % nt})
    for o in range(1, nd):
        pl.semaphore_signal(barrier, inc=1, device_id={"dp": (d + o) % nd})
    pl.semaphore_wait(barrier, nt + nd - 2)

    def part(ch):
        return pl.ds(ch * rows, rows)

    def block(zp, ch, own):
        return grad_ref.at[part(ch)] if own else zbuf.at[zp, ch]

    def up(zp, ch, own):
        return pltpu.make_async_remote_copy(
            block(zp, ch, own), zbuf.at[zp, ch], up_send.at[zp, ch], z_recv.at[zp, ch],
            device_id={"tensor": t + CORES},
        )

    def down(zp, ch, own):
        return pltpu.make_async_remote_copy(
            block(zp, ch, own), zbuf.at[zp, ch], down_send.at[zp, ch], z_recv.at[zp, ch],
            device_id={"tensor": t - CORES},
        )

    def to_owner(zp, ch, own):
        return pltpu.make_async_remote_copy(
            block(zp, ch, own), g.at[ch, c, d], d_send.at[zp, ch], d_recv.at[d, ch],
            device_id={"dp": zp},
        )

    def keep_partner(zp, ch, own):
        return pltpu.make_async_remote_copy(
            block(zp, ch, own), g.at[ch, c, d], own_send.at[ch], p_recv.at[d, ch],
            device_id={"tensor": partner},
        )

    def to_partner(src, ch):
        return pltpu.make_async_remote_copy(
            g.at[ch, c, src], g.at[ch, c, src], p_send.at[src, ch], p_recv.at[src, ch],
            device_id={"tensor": partner},
        )

    def spread(zp, ch, own):
        @pl.when(zp == d)
        def _():
            keep_partner(zp, ch, own).start()
            g[ch, c, d] = grad_ref[part(ch)] if own else zbuf[zp, ch]

        @pl.when(zp != d)
        def _():
            to_owner(zp, ch, own).start()

    def spread_done(zp, ch, own):
        @pl.when(zp == d)
        def _():
            keep_partner(zp, ch, own).wait_send()

        @pl.when(zp != d)
        def _():
            to_owner(zp, ch, own).wait_send()

    def pass_on(ch):
        for o in range(1, nd):
            src = (d + o) % nd
            pltpu.make_async_remote_copy(
                g.at[ch, c, src], g.at[ch, c, src], p_send.at[src, ch], d_recv.at[src, ch],
                device_id={"tensor": partner},
            ).wait_recv()
            to_partner(src, ch).start()

    def att_send(way, ch):
        return pltpu.make_async_remote_copy(
            a.at[d, part(ch)], a.at[d, part(ch)], a_send.at[way, ch], a_recv.at[0, d, ch],
            device_id={"dp": (xn, yn)[way]},
        )

    def att_relay(way, ch):
        src = (xn, yn)[way]
        half = (alpha, beta)[way]
        return pltpu.make_async_remote_copy(
            a.at[src, part(ch), half], a.at[src, part(ch), half], f_send.at[way, ch],
            a_recv.at[1 + way, src, ch], device_id={"dp": (yn, xn)[way]},
        )

    def att_pass(ch):
        for way in range(2):
            src = (xn, yn)[way]
            pltpu.make_async_remote_copy(
                a.at[src, part(ch)], a.at[src, part(ch)], a_send.at[way, ch],
                a_recv.at[0, src, ch], device_id={"dp": src},
            ).wait_recv()
            att_relay(way, ch).start()

    def att_wait(ch):
        for way in range(2):
            half = (alpha, beta)[way]
            pltpu.make_async_remote_copy(
                a.at[dg, part(ch), half], a.at[dg, part(ch), half], f_send.at[way, ch],
                a_recv.at[1 + way, dg, ch], device_id={"dp": (yn, xn)[way]},
            ).wait_recv()

    def first_hop(way, which, ch):
        near = (xn, yn)[way]
        half = (alpha, beta)[way]
        dest = (near, dg)[which]
        return pltpu.make_async_remote_copy(
            partial.at[ch, dest, :, half], r1.at[ch, which, :, half], s1_send.at[way, which, ch],
            s1_recv.at[way, which, ch], device_id={"dp": near},
        )

    def second_hop(way, ch):
        half = (alpha, beta)[way]
        return pltpu.make_async_remote_copy(
            mid.at[ch, :, half], r2.at[ch, :, half], s2_send.at[way, ch], s2_recv.at[way, ch],
            device_id={"dp": (yn, xn)[way]},
        )

    def cast_weight(i):
        fetch_w[i].wait()
        wh[pl.ds(i * tile, tile)] = stage[i % 2].astype(jnp.bfloat16)
        if i + 2 < tiles:
            fetch_w[i + 2].start()

    def project(ch):
        span = 256

        def body(n, carry):
            cols = pl.ds(pl.multiple_of(n * span, span), span)
            acc = None
            for p in range(CORES):
                lhs = g[ch, p].reshape(nd * rows, width)
                term = jnp.dot(
                    lhs, wh[pl.ds(p * width, width), cols], preferred_element_type=jnp.float32
                )
                acc = term if acc is None else acc + term
            partial[ch, :, :, cols] = acc.astype(jnp.bfloat16).reshape(nd, rows, span)
            return carry

        lax.fori_loop(0, width // span, body, 0)

    def turn(ch):
        def body(s, carry):
            at = pl.ds(pl.multiple_of(s * length + ch * rows, rows), rows)
            for p in range(CORES):
                gt[pl.ds(p * width, width), at] = g[ch, p, s].T
            return carry

        lax.fori_loop(0, nd, body, 0)

    def attend_fwd():
        kv = pl.multiple_of(t * heads // (H // KVH) * HD, HD)
        kv_k[...] = k_ref[:, pl.ds(kv, HD)]
        kv_v[...] = v_ref[:, pl.ds(kv, HD)]

        def body(h, carry):
            lanes = pl.ds(pl.multiple_of(h * HD, HD), HD)
            scores = lax.dot_general(
                q_ref[:, lanes], kv_k[...], (((1,), (1,)), ((), ())),
                preferred_element_type=jnp.float32,
            ) * scale
            future = lax.broadcasted_iota(jnp.int32, (length, length), 1) > (
                lax.broadcasted_iota(jnp.int32, (length, length), 0)
            )
            scores = jnp.where(future, -1e30, scores)
            exponent = jnp.exp(scores - jnp.max(scores, axis=-1, keepdims=True))
            probs = exponent / jnp.sum(exponent, axis=-1, keepdims=True)
            prob[h] = probs
            out = jnp.dot(
                probs.astype(jnp.bfloat16), kv_v[...], preferred_element_type=jnp.float32
            )
            a[d, :, lanes] = out.astype(jnp.bfloat16)
            return carry

        lax.fori_loop(0, heads, body, 0)

    def attend_bwd(ch):
        def body(h, carry):
            lanes = pl.ds(pl.multiple_of(h * HD, HD), HD)
            grad = (
                partial[ch, d, :, lanes].astype(jnp.float32)
                + r1[ch, 0, :, lanes].astype(jnp.float32)
                + r2[ch, :, lanes].astype(jnp.float32)
            ).astype(jnp.bfloat16)
            grad_probs = lax.dot_general(
                grad, kv_v[...], (((1,), (1,)), ((), ())), preferred_element_type=jnp.float32
            )
            row_dot = jnp.sum(
                grad.astype(jnp.float32) * a[d, part(ch), lanes].astype(jnp.float32),
                axis=-1, keepdims=True,
            )
            grad_scores = (prob[h, part(ch)] * (grad_probs - row_dot)).astype(jnp.bfloat16)
            out = jnp.dot(grad_scores, kv_k[...], preferred_element_type=jnp.float32) * scale
            gq_ref[part(ch), lanes] = out.astype(jnp.bfloat16)
            return carry

        lax.fori_loop(0, heads, body, 0)

    def column(row):
        return jnp.broadcast_to(row, (HD, HD)).T

    def scales():
        for k in range(total // HD):
            rb1[pl.ds(k * HD, HD)] = column(fr_ref[pl.ds(k, 1)] * beta_first)
            rb2[pl.ds(k * HD, HD)] = column(sr_ref[pl.ds(k, 1)] * beta_second)
        cacc[...] = jnp.zeros_like(cacc)

    def moments(i):
        at = pl.ds(i * tile, tile)
        span = 256

        def body(n, carry):
            high1, high2 = carry
            start = pl.multiple_of(n * span, span)
            grad = jnp.dot(
                gt[at], a[:, :, pl.ds(start, span)].reshape(nd * length, span),
                preferred_element_type=jnp.float32,
            )
            for j in range(span // HD):
                lanes = pl.ds(pl.multiple_of(start + j * HD, HD), HD)
                dw = grad[:, j * HD : (j + 1) * HD]
                first = fcv[at, lanes].astype(jnp.float32) * jnp.minimum(
                    rb1[at], fcol_ref[:, lanes] * beta_first
                ) + (1.0 - beta_first) * dw
                second = scv[at, lanes].astype(jnp.float32) * jnp.minimum(
                    rb2[at], scol_ref[:, lanes] * beta_second
                ) + (1.0 - beta_second) * dw * dw
                fcv[at, lanes] = first.astype(jnp.bfloat16)
                scv[at, lanes] = second.astype(jnp.bfloat16)
                first, second = jnp.abs(first), jnp.abs(second)
                high1 = jnp.maximum(high1, first)
                high2 = jnp.maximum(high2, second)
                cacc[0, :, lanes] = jnp.maximum(
                    cacc[0, :, lanes], jnp.max(first.reshape(tile // 8, 8, HD), axis=0)
                )
                cacc[1, :, lanes] = jnp.maximum(
                    cacc[1, :, lanes], jnp.max(second.reshape(tile // 8, 8, HD), axis=0)
                )
            return high1, high2

        zero = jnp.zeros((tile, HD), jnp.float32)
        high = lax.fori_loop(0, width // span, body, (zero, zero))
        for m in range(2):
            for k in range(tile // HD):
                piece = high[m][k * HD : (k + 1) * HD].T
                rloc[m, pl.ds(i * (tile // HD) + k, 1)] = jnp.max(piece, axis=0, keepdims=True)

    put_out = [
        [
            pltpu.make_async_copy(
                fcv.at[pl.ds(i * tile, tile)], fn_hbm.at[pl.ds(i * tile, tile)], o_sem.at[0, i]
            ),
            pltpu.make_async_copy(
                scv.at[pl.ds(i * tile, tile)], sn_hbm.at[pl.ds(i * tile, tile)], o_sem.at[1, i]
            ),
        ]
        for i in range(tiles)
    ]
    row_copies = [
        pltpu.make_async_remote_copy(
            rloc, rbuf.at[o], rs.at[o], rr.at[o], device_id={"tensor": (t + o) % nt}
        )
        for o in range(1, nt)
    ]
    col_copies = [
        pltpu.make_async_remote_copy(
            cloc, cbuf.at[o], cs.at[o], cr.at[o], device_id={"dp": (d + o) % nd}
        )
        for o in range(1, nd)
    ]

    def reduce_first(ch):
        for which in (1, 0):
            for way in range(2):
                first_hop(way, which, ch).start()

    def reduce_mid(ch):
        for way in range(2):
            half = (alpha, beta)[way]
            first_hop(way, 1, ch).wait_recv()
            mid[ch, :, half] = (
                partial[ch, (yn, xn)[way], :, half].astype(jnp.float32)
                + r1[ch, 1, :, half].astype(jnp.float32)
            ).astype(jnp.bfloat16)

    def reduce_next(ch):
        for way in range(2):
            second_hop(way, ch).start()

    def reduce_wait(ch):
        for way in range(2):
            first_hop(way, 0, ch).wait_recv()
            second_hop(way, ch).wait_recv()

    for ch in chunks:

        @pl.when(has_up)
        def _():
            up(z, ch, True).start()

        @pl.when(has_down)
        def _():
            down(z, ch, True).start()

        spread(z, ch, True)

    fetch_c[0].start()
    fetch_c[1].start()
    attend_fwd()
    cast_weight(0)
    cast_weight(1)

    jobs = {
        0: [lambda: cast_weight(2), lambda: cast_weight(3)],
        1: [lambda: cast_weight(4), lambda: cast_weight(5)],
        2: [lambda: cast_weight(6), lambda: cast_weight(7)],
        3: [scales],
    }
    step = 0
    for dist in range(1, nz):
        for ch in chunks:

            @pl.when(z - dist >= 0)
            def _():
                zp = z - dist
                down(zp, ch, False).wait_recv()

                @pl.when(has_up)
                def _():
                    up(zp, ch, False).start()

                spread(zp, ch, False)

            @pl.when(z + dist < nz)
            def _():
                zp = z + dist
                down(zp, ch, False).wait_recv()

                @pl.when(has_down)
                def _():
                    down(zp, ch, False).start()

                spread(zp, ch, False)

            if dist == 1:
                att_send(0, ch).start()
                att_send(1, ch).start()

            @pl.when(far == dist - 1)
            def _():
                pass_on(ch)

            if dist == 3:
                att_pass(ch)
            for job in jobs.get(step, []):
                job()
            step += 1
    last = nz - 1

    def gathered(ch):
        @pl.when(far == last)
        def _():
            pass_on(ch)

        for src in range(nd):
            pltpu.make_async_remote_copy(
                g.at[ch, 1 - c, src], g.at[ch, 1 - c, src], p_send.at[src, ch],
                p_recv.at[src, ch], device_id={"tensor": partner},
            ).wait_recv()

    for ch in chunks:
        gathered(ch)
        project(ch)
        turn(ch)
        reduce_first(ch)
    for copy in fetch_c:
        copy.wait()
    for ch in chunks:
        att_wait(ch)
    after = {2: lambda: reduce_mid(0), 3: lambda: reduce_next(0), 4: lambda: reduce_mid(1),
             5: lambda: reduce_next(1), 6: lambda: reduce_mid(2), 7: lambda: reduce_next(2)}
    for i in range(tiles):
        moments(i)
        if i in after:
            after[i]()
        if i:
            put_out[i - 1][0].start()
            put_out[i - 1][1].start()
    for m in range(2):
        cloc[pl.ds(m, 1)] = jnp.max(cacc[m], axis=0, keepdims=True)
    put_out[tiles - 1][0].start()
    put_out[tiles - 1][1].start()
    for copy in row_copies + col_copies:
        copy.start()
    for ch in chunks[:-1]:
        reduce_wait(ch)
        attend_bwd(ch)
    for copy in row_copies + col_copies:
        copy.wait()
    high = rloc[...]
    for o in range(1, nt):
        high = jnp.maximum(high, rbuf[o])
    rmax_ref[...] = high
    high = cloc[...]
    for o in range(1, nd):
        high = jnp.maximum(high, cbuf[o])
    cmax_ref[...] = high
    reduce_wait(PARTS - 1)
    attend_bwd(PARTS - 1)

    for ch in chunks:

        @pl.when(has_up)
        def _():
            up(z, ch, True).wait_send()

        @pl.when(has_down)
        def _():
            down(z, ch, True).wait_send()

        spread_done(z, ch, True)
        for dist in range(1, nz):

            @pl.when(z - dist >= 0)
            def _():
                @pl.when(has_up)
                def _():
                    up(z - dist, ch, False).wait_send()

                spread_done(z - dist, ch, False)

            @pl.when(z + dist < nz)
            def _():
                @pl.when(has_down)
                def _():
                    down(z + dist, ch, False).wait_send()

                spread_done(z + dist, ch, False)

        for o in range(1, nd):
            to_partner((d + o) % nd, ch).wait_send()
        for way in range(2):
            att_send(way, ch).wait_send()
            att_relay(way, ch).wait_send()
            first_hop(way, 0, ch).wait_send()
            first_hop(way, 1, ch).wait_send()
            second_hop(way, ch).wait_send()
    for pair in put_out:
        pair[0].wait()
        pair[1].wait()


def fused(queries, keys, values, grad_out, weight, first_code, second_code,
          first_rows, first_cols, second_rows, second_cols, nd, nz):
    length, width = grad_out.shape
    total = weight.shape[0]
    rows = length // PARTS
    heads = width // HD
    nt = CORES * nz
    tile = 256
    tiles = total // tile
    half = jnp.bfloat16
    single = jnp.float32
    dma = pltpu.SemaphoreType.DMA
    vmem = pltpu.VMEM
    inside = pl.BlockSpec(memory_space=pltpu.VMEM)
    outside = pl.BlockSpec(memory_space=pl.ANY)
    blocks = total // HD
    return pl.pallas_call(
        functools.partial(fused_kernel, nd, nz),
        out_shape=(
            jax.ShapeDtypeStruct((length, width), half),
            jax.ShapeDtypeStruct((total, width), half),
            jax.ShapeDtypeStruct((total, width), half),
            jax.ShapeDtypeStruct((2, blocks, HD), single),
            jax.ShapeDtypeStruct((2, width), single),
        ),
        in_specs=[inside] * 4 + [outside] * 3 + [inside] * 4,
        out_specs=(inside, outside, outside, inside, inside),
        scratch_shapes=[
            vmem((nz, PARTS, rows, width), half),
            vmem((PARTS, CORES, nd, rows, width), half),
            vmem((total, nd * length), half),
            vmem((nd, length, width), half),
            vmem((total, width), half),
            vmem((2, tile, width), single),
            vmem((PARTS, nd, rows, width), half),
            vmem((PARTS, 2, rows, width), half),
            vmem((PARTS, rows, width), half),
            vmem((PARTS, rows, width), half),
            vmem((heads, length, length), single),
            vmem((total, width), half),
            vmem((total, width), half),
            vmem((total, HD), single),
            vmem((total, HD), single),
            vmem((2, blocks, HD), single),
            vmem((2, width), single),
            vmem((2, 8, width), single),
            vmem((nt, 2, blocks, HD), single),
            vmem((nd, 2, width), single),
            vmem((length, HD), half),
            vmem((length, HD), half),
            dma((nz, PARTS)),
            dma((nz, PARTS)),
            dma((nz, PARTS)),
            dma((PARTS,)),
            dma((nz, PARTS)),
            dma((nd, PARTS)),
            dma((nd, PARTS)),
            dma((nd, PARTS)),
            dma((2, PARTS)),
            dma((3, nd, PARTS)),
            dma((2, PARTS)),
            dma((2, 2, PARTS)),
            dma((2, 2, PARTS)),
            dma((2, PARTS)),
            dma((2, PARTS)),
            dma((2,)),
            dma((2,)),
            dma((2, tiles)),
            dma((nt,)),
            dma((nt,)),
            dma((nd,)),
            dma((nd,)),
        ],
        compiler_params=pltpu.CompilerParams(
            collective_id=2, has_side_effects=True, vmem_limit_bytes=66 * 1024 * 1024
        ),
    )(
        queries, keys, values, grad_out, weight, first_code, second_code,
        first_rows.reshape(blocks, HD), first_cols.reshape(1, width),
        second_rows.reshape(blocks, HD), second_cols.reshape(1, width),
    )


def finish_kernel(fn_ref, sn_ref, w_ref, rmax_ref, cmax_ref, nw_ref, f_ref, s_ref):
    rows, width = fn_ref.shape
    i = pl.program_id(0)
    count = rows // HD
    for k in range(count):
        at = pl.ds(k * HD, HD)

        def column(m):
            row = 1.0 / (rmax_ref[m, pl.ds(i * count + k, 1)] + code_eps)
            return jnp.broadcast_to(row, (HD, HD)).T

        col1, col2 = column(0), column(1)
        for j in range(width // HD):
            lanes = pl.ds(j * HD, HD)
            first = fn_ref[at, lanes].astype(jnp.float32)
            second = sn_ref[at, lanes].astype(jnp.float32)
            weight = w_ref[at, lanes]
            step = first / correct_first / (jnp.sqrt(second / correct_second) + adam_eps)
            nw_ref[at, lanes] = weight - learning * (step + decay_rate * weight)
            inv1 = 1.0 / (cmax_ref[0:1, lanes] + code_eps)
            inv2 = 1.0 / (cmax_ref[1:2, lanes] + code_eps)
            f_ref[at, lanes] = (first * jnp.maximum(col1, inv1)).astype(jnp.bfloat16)
            s_ref[at, lanes] = (second * jnp.maximum(col2, inv2)).astype(jnp.bfloat16)


def finish(first, second, weight, rmax, cmax):
    total, width = weight.shape
    tile = 256
    big = pl.BlockSpec((tile, width), lambda i: (i, 0))
    whole = lambda x: pl.BlockSpec(x.shape, lambda i: (0,) * x.ndim)
    return pl.pallas_call(
        finish_kernel,
        grid=(total // tile,),
        in_specs=[big, big, big, whole(rmax), whole(cmax)],
        out_specs=(big, big, big),
        out_shape=(
            jax.ShapeDtypeStruct(weight.shape, jnp.float32),
            jax.ShapeDtypeStruct(weight.shape, jnp.bfloat16),
            jax.ShapeDtypeStruct(weight.shape, jnp.bfloat16),
        ),
    )(first, second, weight, rmax, cmax)


def per_device(
    queries,
    keys,
    values,
    grad_out,
    weight,
    first_code,
    first_rows,
    first_cols,
    second_code,
    second_rows,
    second_cols,
):
    dp_count = lax.axis_size("dp")
    cols_dev = queries.shape[1]
    heads_dev = cols_dev // HD
    rows_dev = weight.shape[0]
    width_pad = dp_count * rows_dev
    tensor_count, feats = lax.axis_size("tensor"), grad_out.shape[1]
    if (
        dp_count == 4
        and tensor_count == CORES * dp_count
        and rows_dev == CORES * feats
        and rows_dev % 256 == 0
        and queries.shape[0] == PARTS * HD
    ):
        grad_queries, first, second, rmax, cmax = fused(
            queries, keys, values, grad_out, weight, first_code, second_code,
            first_rows, first_cols, second_rows, second_cols, dp_count, tensor_count // CORES,
        )
        new_weight, first, second = finish(first, second, weight, rmax, cmax)
        return (
            grad_queries,
            new_weight,
            first,
            rmax[0].reshape(rows_dev),
            cmax[0],
            second,
            rmax[1].reshape(rows_dev),
            cmax[1],
        )
    tensor_index = lax.axis_index("tensor")
    kv_start = tensor_index * heads_dev // (H // KVH) * HD
    weight_half = weight.astype(jnp.bfloat16)
    length = queries.shape[0]
    key_sel = lax.dynamic_slice_in_dim(keys, kv_start, HD, 1)
    value_sel = lax.dynamic_slice_in_dim(values, kv_start, HD, 1)
    probabilities, attended = attend(queries, key_sel, value_sel, heads_dev)
    flat = lax.all_gather(grad_out, "tensor", axis=1, tiled=True)
    flat = jnp.pad(flat, ((0, 0), (0, width_pad - flat.shape[1])))
    blocks = jnp.moveaxis(flat.reshape(length, dp_count, 1, rows_dev), 0, 2)
    mine = lax.all_to_all(blocks, "dp", 0, 0, tiled=True)
    all_attended = lax.all_gather(attended, "dp", axis=0, tiled=True)
    mine = mine[:, 0].reshape(dp_count * length, rows_dev)
    partial = jnp.dot(mine, weight_half, preferred_element_type=jnp.float32)
    partial, all_attended = lax.optimization_barrier(
        (partial.astype(jnp.bfloat16), all_attended)
    )
    grad_half = lax.psum_scatter(
        partial, "dp", scatter_dimension=0, tiled=True
    )
    weight_grad = jnp.einsum(
        "sc,sh->ch", mine, all_attended, preferred_element_type=jnp.float32
    )
    grad_queries = attend_back(probabilities, attended, grad_half, key_sel, value_sel, heads_dev)
    first = first_code.astype(jnp.float32) * jnp.minimum(first_rows[:, None], first_cols[None, :])
    second = second_code.astype(jnp.float32) * jnp.minimum(
        second_rows[:, None], second_cols[None, :]
    )
    first_new = beta_first * first + (1.0 - beta_first) * weight_grad
    second_new = beta_second * second + (1.0 - beta_second) * weight_grad * weight_grad
    step_size = first_new / correct_first / (jnp.sqrt(second_new / correct_second) + adam_eps)
    new_weight = weight - learning * (step_size + decay_rate * weight)
    first_abs = jnp.abs(first_new)
    second_abs = jnp.abs(second_new)
    local_rows_max = jnp.stack([jnp.max(first_abs, axis=1), jnp.max(second_abs, axis=1)])
    local_cols_max = jnp.stack([jnp.max(first_abs, axis=0), jnp.max(second_abs, axis=0)])
    rows_mine, cols_mine = maxima(local_rows_max, local_cols_max, dp_count, tensor_count)
    next_first_code = (
        first_new / (jnp.minimum(rows_mine[0][:, None], cols_mine[0][None, :]) + code_eps)
    ).astype(jnp.bfloat16)
    next_second_code = (
        second_new / (jnp.minimum(rows_mine[1][:, None], cols_mine[1][None, :]) + code_eps)
    ).astype(jnp.bfloat16)
    return (
        grad_queries,
        new_weight,
        next_first_code,
        rows_mine[0],
        cols_mine[0],
        next_second_code,
        rows_mine[1],
        cols_mine[1],
    )


def solution(mesh):
    return jax.shard_map(
        per_device,
        mesh=mesh,
        in_specs=(
            P("dp", "tensor"),
            P("dp", None),
            P("dp", None),
            P("dp", "tensor"),
            P("dp", "tensor"),
            P("dp", "tensor"),
            P("dp"),
            P("tensor"),
            P("dp", "tensor"),
            P("dp"),
            P("tensor"),
        ),
        out_specs=(
            P("dp", "tensor"),
            P("dp", "tensor"),
            P("dp", "tensor"),
            P("dp"),
            P("tensor"),
            P("dp", "tensor"),
            P("dp"),
            P("tensor"),
        ),
        check_vma=False,
    )
```

```python
import functools

import jax
import jax.numpy as jnp
from jax import lax
from jax.experimental import pallas as pl
from jax.experimental.pallas import tpu as pltpu
from jax.sharding import PartitionSpec as P

H = 64
KVH = 8
HD = 128


beta_first = 0.9
beta_second = 0.95
learning = 0.01
decay_rate = 0.1
adam_eps = 1e-08
code_eps = 1e-06
correct_first = 1.0 - 0.9**10
correct_second = 1.0 - 0.95**10


def attend(queries, key_sel, value_sel, heads_dev):
    length = queries.shape[0]
    query_heads = queries.reshape(length, heads_dev, HD)
    scores = jnp.einsum(
        "qhd,kd->hqk", query_heads, key_sel, preferred_element_type=jnp.float32
    ) * HD ** (-0.5)
    future = lax.broadcasted_iota(jnp.int32, (length, length), 1) > lax.broadcasted_iota(
        jnp.int32, (length, length), 0
    )
    scores = jnp.where(future[None], -1e30, scores)
    highest = jnp.max(scores, axis=-1, keepdims=True)
    exponent = jnp.exp(scores - highest)
    probabilities = exponent / jnp.sum(exponent, axis=-1, keepdims=True)
    weights_half = probabilities.astype(jnp.bfloat16)
    attended = jnp.einsum(
        "hqk,kd->qhd", weights_half, value_sel, preferred_element_type=jnp.float32
    )
    return (probabilities, attended.astype(jnp.bfloat16).reshape(length, heads_dev * HD))


def attend_back(probabilities, attended, grad_half, key_sel, value_sel, heads_dev):
    length = grad_half.shape[0]
    grad_heads = grad_half.reshape(length, heads_dev, HD)
    grad_probs = jnp.einsum(
        "qhd,kd->hqk", grad_heads, value_sel, preferred_element_type=jnp.float32
    )
    row_dot = jnp.sum(
        grad_heads.astype(jnp.float32)
        * attended.reshape(length, heads_dev, HD).astype(jnp.float32),
        axis=-1,
    )
    grad_scores = (probabilities * (grad_probs - row_dot.T[:, :, None])).astype(jnp.bfloat16)
    grad_query = jnp.einsum(
        "hqk,kd->qhd", grad_scores, key_sel, preferred_element_type=jnp.float32
    ) * HD ** (-0.5)
    return grad_query.astype(jnp.bfloat16).reshape(length, heads_dev * HD)


CORES = 2


def maxima_kernel(nd, nt, r_ref, c_ref, ro_ref, co_ref, rbuf, cbuf, rs, rr, cs, cr):
    d = lax.axis_index("dp")
    t = lax.axis_index("tensor")
    barrier = pltpu.get_barrier_semaphore()
    for o in range(1, nt):
        pl.semaphore_signal(barrier, inc=1, device_id={"tensor": (t + o) % nt})
    for o in range(1, nd):
        pl.semaphore_signal(barrier, inc=1, device_id={"dp": (d + o) % nd})
    pl.semaphore_wait(barrier, nt + nd - 2)
    copies = [
        pltpu.make_async_remote_copy(
            r_ref, rbuf.at[o], rs.at[o], rr.at[o], device_id={"tensor": (t + o) % nt}
        )
        for o in range(1, nt)
    ] + [
        pltpu.make_async_remote_copy(
            c_ref, cbuf.at[o], cs.at[o], cr.at[o], device_id={"dp": (d + o) % nd}
        )
        for o in range(1, nd)
    ]
    for copy in copies:
        copy.start()
    for copy in copies:
        copy.wait()
    rows = r_ref[...]
    for o in range(1, nt):
        rows = jnp.maximum(rows, rbuf[o])
    ro_ref[...] = rows
    cols = c_ref[...]
    for o in range(1, nd):
        cols = jnp.maximum(cols, cbuf[o])
    co_ref[...] = cols


def maxima(rows, cols, nd, nt):
    dma = pltpu.SemaphoreType.DMA
    vmem = pl.BlockSpec(memory_space=pltpu.VMEM)
    return pl.pallas_call(
        functools.partial(maxima_kernel, nd, nt),
        out_shape=(
            jax.ShapeDtypeStruct(rows.shape, rows.dtype),
            jax.ShapeDtypeStruct(cols.shape, cols.dtype),
        ),
        in_specs=[vmem] * 2,
        out_specs=(vmem,) * 2,
        scratch_shapes=[
            pltpu.VMEM((nt,) + rows.shape, rows.dtype),
            pltpu.VMEM((nd,) + cols.shape, cols.dtype),
            dma((nt,)),
            dma((nt,)),
            dma((nd,)),
            dma((nd,)),
        ],
        compiler_params=pltpu.CompilerParams(collective_id=1, has_side_effects=True),
    )(rows, cols)


PARTS = 3
SPLIT = 2
SUB = PARTS * SPLIT
LAG = 2
TILE = 256
HALVES = 2


def halves(width):
    return [pl.ds(k * (width // HALVES), width // HALVES) for k in range(HALVES)]


def fused_kernel(
    nd, nz,
    q_ref, k_ref, v_ref, grad_ref, w_hbm, fc_hbm, sc_hbm, fr_ref, fcol_ref, sr_ref, scol_ref,
    gq_ref, nw_ref, fcv, scv, rmax_ref, cmax_ref,
    zbuf, g, gt, a, wh, partial, r1, r2, mid, prob, rb1, rb2, even, odd, racc,
    rloc, cloc, cacc, rbuf, cbuf, kv_k, kv_v,
    up_send, down_send, z_recv, own_send, d_send, d_recv, p_send, p_recv,
    a_send, a_recv, f_send, s1_send, s1_recv, s2_send, s2_recv,
    w_sem, c_sem, rs, rr, cs, cr,
):
    d = lax.axis_index("dp")
    t = lax.axis_index("tensor")
    z = t // CORES
    c = t % CORES
    partner = t + 1 - 2 * c
    xn = d + 1 - 2 * (d % 2)
    yn = (d + 2) % 4
    dg = 3 - d
    length, width = grad_ref.shape
    rows = length // PARTS
    fine = length // SUB
    heads = width // HD
    total = w_hbm.shape[0]
    nt = CORES * nz
    has_up = z < nz - 1
    has_down = z > 0
    tile = TILE
    tiles = total // tile
    alpha, beta = halves(width)
    chunks = range(PARTS)
    subs = range(SUB)
    scale = HD ** (-0.5)

    fetch_w = [
        pltpu.make_async_copy(
            w_hbm.at[pl.ds(i * tile, tile)], nw_ref.at[pl.ds(i * tile, tile)], w_sem.at[i]
        )
        for i in range(tiles)
    ]
    fetch_c = [
        pltpu.make_async_copy(fc_hbm, fcv, c_sem.at[0]),
        pltpu.make_async_copy(sc_hbm, scv, c_sem.at[1]),
    ]
    for copy in fetch_w:
        copy.start()

    barrier = pltpu.get_barrier_semaphore()
    for o in range(1, nt):
        pl.semaphore_signal(barrier, inc=1, device_id={"tensor": (t + o) % nt})
    for o in range(1, nd):
        pl.semaphore_signal(barrier, inc=1, device_id={"dp": (d + o) % nd})
    pl.semaphore_wait(barrier, nt + nd - 2)

    def part(ch):
        return pl.ds(ch * rows, rows)

    def bit(k):
        return pl.ds(k * fine, fine)

    def block(zp, k, own):
        return grad_ref.at[bit(k)] if own else zbuf.at[zp, k]

    def slot(core, src, k):
        return g.at[k // SPLIT, core, src, bit(k % SPLIT)]

    def up(zp, ch, own):
        return pltpu.make_async_remote_copy(
            block(zp, ch, own), zbuf.at[zp, ch], up_send.at[zp, ch], z_recv.at[zp, ch],
            device_id={"tensor": t + CORES},
        )

    def down(zp, ch, own):
        return pltpu.make_async_remote_copy(
            block(zp, ch, own), zbuf.at[zp, ch], down_send.at[zp, ch], z_recv.at[zp, ch],
            device_id={"tensor": t - CORES},
        )

    def to_owner(zp, ch, own):
        return pltpu.make_async_remote_copy(
            block(zp, ch, own), slot(c, d, ch), d_send.at[zp, ch], d_recv.at[d, ch],
            device_id={"dp": zp},
        )

    def keep_partner(zp, ch, own):
        return pltpu.make_async_remote_copy(
            block(zp, ch, own), slot(c, d, ch), own_send.at[ch], p_recv.at[d, ch],
            device_id={"tensor": partner},
        )

    def to_partner(src, ch):
        return pltpu.make_async_remote_copy(
            slot(c, src, ch), slot(c, src, ch), p_send.at[src, ch], p_recv.at[src, ch],
            device_id={"tensor": partner},
        )

    def spread(zp, ch, own):
        @pl.when(zp == d)
        def _():
            keep_partner(zp, ch, own).start()
            g[ch // SPLIT, c, d, bit(ch % SPLIT)] = grad_ref[bit(ch)] if own else zbuf[zp, ch]

        @pl.when(zp != d)
        def _():
            to_owner(zp, ch, own).start()

    def spread_done(zp, ch, own):
        @pl.when(zp == d)
        def _():
            keep_partner(zp, ch, own).wait_send()

        @pl.when(zp != d)
        def _():
            to_owner(zp, ch, own).wait_send()

    def pass_on(ch):
        for o in range(1, nd):
            src = (d + o) % nd
            pltpu.make_async_remote_copy(
                slot(c, src, ch), slot(c, src, ch), p_send.at[src, ch], d_recv.at[src, ch],
                device_id={"tensor": partner},
            ).wait_recv()
            to_partner(src, ch).start()

    def att_send(way, ch):
        return pltpu.make_async_remote_copy(
            a.at[d, bit(ch)], a.at[d, bit(ch)], a_send.at[way, ch], a_recv.at[0, d, ch],
            device_id={"dp": (xn, yn)[way]},
        )

    def att_relay(way, ch):
        src = (xn, yn)[way]
        half = (alpha, beta)[way]
        return pltpu.make_async_remote_copy(
            a.at[src, bit(ch), half], a.at[src, bit(ch), half], f_send.at[way, ch],
            a_recv.at[1 + way, src, ch], device_id={"dp": (yn, xn)[way]},
        )

    def att_pass(ch):
        for way in range(2):
            src = (xn, yn)[way]
            pltpu.make_async_remote_copy(
                a.at[src, bit(ch)], a.at[src, bit(ch)], a_send.at[way, ch],
                a_recv.at[0, src, ch], device_id={"dp": src},
            ).wait_recv()
            att_relay(way, ch).start()

    def att_wait(ch):
        for way in range(2):
            half = (alpha, beta)[way]
            pltpu.make_async_remote_copy(
                a.at[dg, bit(ch), half], a.at[dg, bit(ch), half], f_send.at[way, ch],
                a_recv.at[1 + way, dg, ch], device_id={"dp": (yn, xn)[way]},
            ).wait_recv()

    def first_hop(way, which, ch):
        near = (xn, yn)[way]
        half = (alpha, beta)[way]
        dest = (near, dg)[which]
        return pltpu.make_async_remote_copy(
            partial.at[ch, dest, :, half], r1.at[ch, which, :, half], s1_send.at[way, which, ch],
            s1_recv.at[way, which, ch], device_id={"dp": near},
        )

    def second_hop(way, ch):
        half = (alpha, beta)[way]
        return pltpu.make_async_remote_copy(
            mid.at[ch, :, half], r2.at[ch, :, half], s2_send.at[way, ch], s2_recv.at[way, ch],
            device_id={"dp": (yn, xn)[way]},
        )

    def cast_weight(i):
        fetch_w[i].wait()
        wh[pl.ds(i * tile, tile)] = nw_ref[pl.ds(i * tile, tile)].astype(jnp.bfloat16)

    def project(ch):
        span = 256

        def body(n, carry):
            cols = pl.ds(pl.multiple_of(n * span, span), span)
            acc = None
            for p in range(CORES):
                lhs = g[ch, p].reshape(nd * rows, width)
                term = jnp.dot(
                    lhs, wh[pl.ds(p * width, width), cols], preferred_element_type=jnp.float32
                )
                acc = term if acc is None else acc + term
            partial[ch, :, :, cols] = acc.astype(jnp.bfloat16).reshape(nd, rows, span)
            return carry

        lax.fori_loop(0, width // span, body, 0)

    def turn(ch):
        def body(s, carry):
            at = pl.ds(pl.multiple_of(s * length + ch * rows, rows), rows)
            for p in range(CORES):
                gt[pl.ds(p * width, width), at] = g[ch, p, s].T
            return carry

        lax.fori_loop(0, nd, body, 0)

    def attend_fwd():
        kv = pl.multiple_of(t * heads // (H // KVH) * HD, HD)
        kv_k[...] = k_ref[:, pl.ds(kv, HD)]
        kv_v[...] = v_ref[:, pl.ds(kv, HD)]

        def body(h, carry):
            lanes = pl.ds(pl.multiple_of(h * HD, HD), HD)
            scores = lax.dot_general(
                q_ref[:, lanes], kv_k[...], (((1,), (1,)), ((), ())),
                preferred_element_type=jnp.float32,
            ) * scale
            future = lax.broadcasted_iota(jnp.int32, (length, length), 1) > (
                lax.broadcasted_iota(jnp.int32, (length, length), 0)
            )
            scores = jnp.where(future, -1e30, scores)
            exponent = jnp.exp(scores - jnp.max(scores, axis=-1, keepdims=True))
            probs = exponent / jnp.sum(exponent, axis=-1, keepdims=True)
            prob[h] = probs
            out = jnp.dot(
                probs.astype(jnp.bfloat16), kv_v[...], preferred_element_type=jnp.float32
            )
            a[d, :, lanes] = out.astype(jnp.bfloat16)
            return carry

        lax.fori_loop(0, heads, body, 0)

    def attend_bwd(ch):
        def body(h, carry):
            lanes = pl.ds(pl.multiple_of(h * HD, HD), HD)
            grad = (
                partial[ch, d, :, lanes].astype(jnp.float32)
                + r1[ch, 0, :, lanes].astype(jnp.float32)
                + r2[ch, :, lanes].astype(jnp.float32)
            ).astype(jnp.bfloat16)
            grad_probs = lax.dot_general(
                grad, kv_v[...], (((1,), (1,)), ((), ())), preferred_element_type=jnp.float32
            )
            row_dot = jnp.sum(
                grad.astype(jnp.float32) * a[d, part(ch), lanes].astype(jnp.float32),
                axis=-1, keepdims=True,
            )
            grad_scores = (prob[h, part(ch)] * (grad_probs - row_dot)).astype(jnp.bfloat16)
            out = jnp.dot(grad_scores, kv_k[...], preferred_element_type=jnp.float32) * scale
            gq_ref[part(ch), lanes] = out.astype(jnp.bfloat16)
            return carry

        lax.fori_loop(0, heads, body, 0)

    def column(row):
        return jnp.broadcast_to(row, (HD, HD)).T

    def scales():
        for k in range(total // HD):
            rb1[pl.ds(k * HD, HD)] = column(fr_ref[pl.ds(k, 1)] * beta_first)
            rb2[pl.ds(k * HD, HD)] = column(sr_ref[pl.ds(k, 1)] * beta_second)
        cacc[...] = jnp.zeros_like(cacc)
        racc[...] = jnp.zeros_like(racc)

    tall, span = even.shape
    across = width // span
    pieces = (total // tall) * across

    def place(it):
        return (
            pl.ds(pl.multiple_of(it // across * tall, tall), tall),
            pl.multiple_of(it % across * span, span),
        )

    def gradient(it, out):
        at, start = place(it)
        out[...] = jnp.dot(
            gt[at], a[:, :, pl.ds(start, span)].reshape(nd * length, span),
            preferred_element_type=jnp.float32,
        )

    def moments(it, grad):
        at, start = place(it)
        for j in range(span // HD):
            lanes = pl.ds(pl.multiple_of(start + j * HD, HD), HD)
            dw = grad[:, j * HD : (j + 1) * HD]
            first = fcv[at, lanes].astype(jnp.float32) * jnp.minimum(
                rb1[at], fcol_ref[:, lanes] * beta_first
            ) + (1.0 - beta_first) * dw
            second = scv[at, lanes].astype(jnp.float32) * jnp.minimum(
                rb2[at], scol_ref[:, lanes] * beta_second
            ) + (1.0 - beta_second) * dw * dw
            fcv[at, lanes] = first.astype(jnp.bfloat16)
            scv[at, lanes] = second.astype(jnp.bfloat16)
            for m, value in enumerate((jnp.abs(first), jnp.abs(second))):
                racc[m, at] = jnp.maximum(racc[m, at], value)
                cacc[m, :, lanes] = jnp.maximum(
                    cacc[m, :, lanes], jnp.max(value.reshape(tall // 8, 8, HD), axis=0)
                )

    def pair(n, carry):
        gradient(2 * n + 1, odd)
        moments(2 * n, even)
        gradient(jnp.minimum(2 * n + 2, pieces - 1), even)
        moments(2 * n + 1, odd)
        return carry

    def row_high():
        for m in range(2):
            for k in range(total // HD):
                piece = racc[m, pl.ds(k * HD, HD)].T
                rloc[m, pl.ds(k, 1)] = jnp.max(piece, axis=0, keepdims=True)

    def weight_step(i):
        def body(n, carry):
            at = pl.ds(pl.multiple_of(i * tile + n * 32, 32), 32)
            first = fcv[at].astype(jnp.float32)
            second = scv[at].astype(jnp.float32)
            root = jnp.sqrt(second * (1.0 / correct_second)) + adam_eps
            nw_ref[at] = (1.0 - learning * decay_rate) * nw_ref[at] - (
                learning / correct_first
            ) * first / root
            return carry

        lax.fori_loop(0, tile // 32, body, 0)

    def codes(i):
        def body(n, carry):
            k = i * (tile // HD) + n
            at = pl.ds(pl.multiple_of(k * HD, HD), HD)
            col1 = column(1.0 / (rmax_ref[0, pl.ds(k, 1)] + code_eps))
            col2 = column(1.0 / (rmax_ref[1, pl.ds(k, 1)] + code_eps))
            for j in range(width // HD):
                lanes = pl.ds(j * HD, HD)
                inv1 = jnp.maximum(col1, cloc[0:1, lanes])
                inv2 = jnp.maximum(col2, cloc[1:2, lanes])
                fcv[at, lanes] = (fcv[at, lanes].astype(jnp.float32) * inv1).astype(jnp.bfloat16)
                scv[at, lanes] = (scv[at, lanes].astype(jnp.float32) * inv2).astype(jnp.bfloat16)
            return carry

        lax.fori_loop(0, tile // HD, body, 0)

    row_copies = [
        pltpu.make_async_remote_copy(
            rloc, rbuf.at[o], rs.at[o], rr.at[o], device_id={"tensor": (t + o) % nt}
        )
        for o in range(1, nt)
    ]
    col_copies = [
        pltpu.make_async_remote_copy(
            cloc, cbuf.at[o], cs.at[o], cr.at[o], device_id={"dp": (d + o) % nd}
        )
        for o in range(1, nd)
    ]

    def reduce_first(ch):
        for which in (1, 0):
            for way in range(2):
                first_hop(way, which, ch).start()

    def reduce_mid(ch):
        for way in range(2):
            half = (alpha, beta)[way]
            first_hop(way, 1, ch).wait_recv()
            mid[ch, :, half] = (
                partial[ch, (yn, xn)[way], :, half].astype(jnp.float32)
                + r1[ch, 1, :, half].astype(jnp.float32)
            ).astype(jnp.bfloat16)

    def reduce_next(ch):
        for way in range(2):
            second_hop(way, ch).start()

    def reduce_wait(ch):
        for way in range(2):
            first_hop(way, 0, ch).wait_recv()
            second_hop(way, ch).wait_recv()

    def send_own(k):
        @pl.when(has_up)
        def _():
            up(z, k, True).start()

        @pl.when(has_down)
        def _():
            down(z, k, True).start()

        spread(z, k, True)

    def forward(dist, k):
        @pl.when(z - dist >= 0)
        def _():
            zp = z - dist
            down(zp, k, False).wait_recv()

            @pl.when(has_up)
            def _():
                up(zp, k, False).start()

            spread(zp, k, False)

        @pl.when(z + dist < nz)
        def _():
            zp = z + dist
            down(zp, k, False).wait_recv()

            @pl.when(has_down)
            def _():
                down(zp, k, False).start()

            spread(zp, k, False)

    def gathered(ch):
        for k in range(ch * SPLIT, (ch + 1) * SPLIT):
            for src in range(nd):
                pltpu.make_async_remote_copy(
                    slot(1 - c, src, k), slot(1 - c, src, k), p_send.at[src, k],
                    p_recv.at[src, k], device_id={"tensor": partner},
                ).wait_recv()

    def att_start(k):
        att_send(0, k).start()
        att_send(1, k).start()

    send_own(0)
    send_own(1)
    fetch_c[0].start()
    fetch_c[1].start()
    attend_fwd()
    cast_weight(0)
    jobs = {
        (0, 1): [lambda: att_start(0), lambda: att_start(1), lambda: cast_weight(1)],
        (0, 2): [lambda: cast_weight(2)],
        (0, 3): [lambda: cast_weight(3)],
        (1, 1): [lambda: att_start(2), lambda: att_start(3), lambda: cast_weight(4)],
        (1, 2): [lambda: cast_weight(5)],
        (1, 3): [lambda: cast_weight(6)],
        (2, 1): [lambda: att_start(4), lambda: att_start(5), lambda: cast_weight(7)],
        (2, 2): [scales],
        (3, 3): [lambda: att_pass(0), lambda: att_pass(1), lambda: att_pass(2)],
        (4, 1): [lambda: gathered(0), lambda: project(0)],
        (4, 2): [lambda: turn(0)],
        (4, 3): [lambda: att_pass(3), lambda: att_pass(4), lambda: att_pass(5),
                 lambda: reduce_first(0)],
        (5, 2): [lambda: gathered(1), lambda: project(1)],
    }
    for k in subs:
        if k >= LAG:
            pass_on(k - LAG)
        for dist in range(1, nz):
            forward(dist, k)
            if dist == 1 and k + 2 < SUB:
                send_own(k + 2)
            for job in jobs.get((k, dist), []):
                job()
    reduce_first(1)
    pass_on(SUB - 2)
    pass_on(SUB - 1)
    turn(1)
    gathered(2)
    project(2)
    reduce_first(2)
    reduce_mid(0)
    turn(2)
    reduce_next(0)
    for copy in fetch_c:
        copy.wait()
    for ch in subs:
        att_wait(ch)
    gradient(0, even)
    reduce_mid(1)
    lax.fori_loop(0, 1, pair, 0)
    reduce_next(1)
    lax.fori_loop(1, pieces // 4, pair, 0)
    reduce_mid(2)
    lax.fori_loop(pieces // 4, pieces // 4 + 1, pair, 0)
    reduce_next(2)
    lax.fori_loop(pieces // 4 + 1, pieces // 2, pair, 0)
    row_high()
    for m in range(2):
        cloc[pl.ds(m, 1)] = jnp.max(cacc[m], axis=0, keepdims=True)
    weight_step(0)
    for copy in row_copies + col_copies:
        copy.start()
    for i in range(1, tiles):
        weight_step(i)
    for ch in chunks[:-1]:
        reduce_wait(ch)
        attend_bwd(ch)
    for copy in row_copies + col_copies:
        copy.wait()
    high = rloc[...]
    for o in range(1, nt):
        high = jnp.maximum(high, rbuf[o])
    rmax_ref[...] = high
    high = cloc[...]
    for o in range(1, nd):
        high = jnp.maximum(high, cbuf[o])
    cmax_ref[...] = high
    cloc[...] = 1.0 / (high + code_eps)
    for i in range(tiles):
        codes(i)
    reduce_wait(2)
    attend_bwd(2)

    for ch in subs:

        @pl.when(has_up)
        def _():
            up(z, ch, True).wait_send()

        @pl.when(has_down)
        def _():
            down(z, ch, True).wait_send()

        spread_done(z, ch, True)
        for dist in range(1, nz):

            @pl.when(z - dist >= 0)
            def _():
                @pl.when(has_up)
                def _():
                    up(z - dist, ch, False).wait_send()

                spread_done(z - dist, ch, False)

            @pl.when(z + dist < nz)
            def _():
                @pl.when(has_down)
                def _():
                    down(z + dist, ch, False).wait_send()

                spread_done(z + dist, ch, False)

        for o in range(1, nd):
            to_partner((d + o) % nd, ch).wait_send()
        for way in range(2):
            att_send(way, ch).wait_send()
            att_relay(way, ch).wait_send()
    for ch in chunks:
        for way in range(2):
            first_hop(way, 0, ch).wait_send()
            first_hop(way, 1, ch).wait_send()
            second_hop(way, ch).wait_send()


def fused(queries, keys, values, grad_out, weight, first_code, second_code,
          first_rows, first_cols, second_rows, second_cols, nd, nz):
    length, width = grad_out.shape
    total = weight.shape[0]
    rows = length // PARTS
    heads = width // HD
    nt = CORES * nz
    tiles = total // TILE
    half = jnp.bfloat16
    single = jnp.float32
    dma = pltpu.SemaphoreType.DMA
    vmem = pltpu.VMEM
    inside = pl.BlockSpec(memory_space=pltpu.VMEM)
    outside = pl.BlockSpec(memory_space=pl.ANY)
    blocks = total // HD
    return pl.pallas_call(
        functools.partial(fused_kernel, nd, nz),
        out_shape=(
            vmem((length, width), half),
            vmem((total, width), single),
            vmem((total, width), half),
            vmem((total, width), half),
            vmem((2, blocks, HD), single),
            vmem((2, width), single),
        ),
        in_specs=[inside] * 4 + [outside] * 3 + [inside] * 4,
        out_specs=(inside,) * 6,
        scratch_shapes=[
            vmem((nz, SUB, length // SUB, width), half),
            vmem((PARTS, CORES, nd, rows, width), half),
            vmem((total, nd * length), half),
            vmem((nd, length, width), half),
            vmem((total, width), half),
            vmem((PARTS, nd, rows, width), half),
            vmem((PARTS, 2, rows, width), half),
            vmem((PARTS, rows, width), half),
            vmem((PARTS, rows, width), half),
            vmem((heads, length, length), single),
            vmem((total, HD), single),
            vmem((total, HD), single),
            vmem((512, 256), single),
            vmem((512, 256), single),
            vmem((2, total, HD), single),
            vmem((2, blocks, HD), single),
            vmem((2, width), single),
            vmem((2, 8, width), single),
            vmem((nt, 2, blocks, HD), single),
            vmem((nd, 2, width), single),
            vmem((length, HD), half),
            vmem((length, HD), half),
            dma((nz, SUB)),
            dma((nz, SUB)),
            dma((nz, SUB)),
            dma((SUB,)),
            dma((nz, SUB)),
            dma((nd, SUB)),
            dma((nd, SUB)),
            dma((nd, SUB)),
            dma((2, SUB)),
            dma((3, nd, SUB)),
            dma((2, SUB)),
            dma((2, 2, PARTS)),
            dma((2, 2, PARTS)),
            dma((2, PARTS)),
            dma((2, PARTS)),
            dma((tiles,)),
            dma((2,)),
            dma((nt,)),
            dma((nt,)),
            dma((nd,)),
            dma((nd,)),
        ],
        compiler_params=pltpu.CompilerParams(
            collective_id=2, has_side_effects=True, vmem_limit_bytes=46 * 1024 * 1024
        ),
    )(
        queries, keys, values, grad_out, weight, first_code, second_code,
        first_rows.reshape(blocks, HD), first_cols.reshape(1, width),
        second_rows.reshape(blocks, HD), second_cols.reshape(1, width),
    )


def per_device(
    queries,
    keys,
    values,
    grad_out,
    weight,
    first_code,
    first_rows,
    first_cols,
    second_code,
    second_rows,
    second_cols,
):
    dp_count = lax.axis_size("dp")
    cols_dev = queries.shape[1]
    heads_dev = cols_dev // HD
    rows_dev = weight.shape[0]
    width_pad = dp_count * rows_dev
    tensor_count, feats = lax.axis_size("tensor"), grad_out.shape[1]
    if (
        dp_count == 4
        and tensor_count == CORES * dp_count
        and rows_dev == CORES * feats
        and rows_dev % 1024 == 0
        and queries.shape[0] == PARTS * HD
    ):
        grad_queries, new_weight, first, second, rmax, cmax = fused(
            queries, keys, values, grad_out, weight, first_code, second_code,
            first_rows, first_cols, second_rows, second_cols, dp_count, tensor_count // CORES,
        )
        return (
            grad_queries,
            new_weight,
            first,
            rmax[0].reshape(rows_dev),
            cmax[0],
            second,
            rmax[1].reshape(rows_dev),
            cmax[1],
        )
    tensor_index = lax.axis_index("tensor")
    kv_start = tensor_index * heads_dev // (H // KVH) * HD
    weight_half = weight.astype(jnp.bfloat16)
    length = queries.shape[0]
    key_sel = lax.dynamic_slice_in_dim(keys, kv_start, HD, 1)
    value_sel = lax.dynamic_slice_in_dim(values, kv_start, HD, 1)
    probabilities, attended = attend(queries, key_sel, value_sel, heads_dev)
    flat = lax.all_gather(grad_out, "tensor", axis=1, tiled=True)
    flat = jnp.pad(flat, ((0, 0), (0, width_pad - flat.shape[1])))
    blocks = jnp.moveaxis(flat.reshape(length, dp_count, 1, rows_dev), 0, 2)
    mine = lax.all_to_all(blocks, "dp", 0, 0, tiled=True)
    all_attended = lax.all_gather(attended, "dp", axis=0, tiled=True)
    mine = mine[:, 0].reshape(dp_count * length, rows_dev)
    partial = jnp.dot(mine, weight_half, preferred_element_type=jnp.float32)
    partial, all_attended = lax.optimization_barrier(
        (partial.astype(jnp.bfloat16), all_attended)
    )
    grad_half = lax.psum_scatter(
        partial, "dp", scatter_dimension=0, tiled=True
    )
    weight_grad = jnp.einsum(
        "sc,sh->ch", mine, all_attended, preferred_element_type=jnp.float32
    )
    grad_queries = attend_back(probabilities, attended, grad_half, key_sel, value_sel, heads_dev)
    first = first_code.astype(jnp.float32) * jnp.minimum(first_rows[:, None], first_cols[None, :])
    second = second_code.astype(jnp.float32) * jnp.minimum(
        second_rows[:, None], second_cols[None, :]
    )
    first_new = beta_first * first + (1.0 - beta_first) * weight_grad
    second_new = beta_second * second + (1.0 - beta_second) * weight_grad * weight_grad
    step_size = first_new / correct_first / (jnp.sqrt(second_new / correct_second) + adam_eps)
    new_weight = weight - learning * (step_size + decay_rate * weight)
    first_abs = jnp.abs(first_new)
    second_abs = jnp.abs(second_new)
    local_rows_max = jnp.stack([jnp.max(first_abs, axis=1), jnp.max(second_abs, axis=1)])
    local_cols_max = jnp.stack([jnp.max(first_abs, axis=0), jnp.max(second_abs, axis=0)])
    rows_mine, cols_mine = maxima(local_rows_max, local_cols_max, dp_count, tensor_count)
    next_first_code = (
        first_new / (jnp.minimum(rows_mine[0][:, None], cols_mine[0][None, :]) + code_eps)
    ).astype(jnp.bfloat16)
    next_second_code = (
        second_new / (jnp.minimum(rows_mine[1][:, None], cols_mine[1][None, :]) + code_eps)
    ).astype(jnp.bfloat16)
    return (
        grad_queries,
        new_weight,
        next_first_code,
        rows_mine[0],
        cols_mine[0],
        next_second_code,
        rows_mine[1],
        cols_mine[1],
    )


def solution(mesh):
    return jax.shard_map(
        per_device,
        mesh=mesh,
        in_specs=(
            P("dp", "tensor"),
            P("dp", None),
            P("dp", None),
            P("dp", "tensor"),
            P("dp", "tensor"),
            P("dp", "tensor"),
            P("dp"),
            P("tensor"),
            P("dp", "tensor"),
            P("dp"),
            P("tensor"),
        ),
        out_specs=(
            P("dp", "tensor"),
            P("dp", "tensor"),
            P("dp", "tensor"),
            P("dp"),
            P("tensor"),
            P("dp", "tensor"),
            P("dp"),
            P("tensor"),
        ),
        check_vma=False,
    )
```
